32 devices in a mesh: dp: 1 (over z), ep_b: 4 (over y), ep_a: 8 (over x, core).
Axes of the slice: x: 4, y: 4, z: 1, core: 2. Of those that a mesh axis runs over, the one named last changes fastest.
The devices are a block of a 4x4x8 slice.
Arguments:
- tokens: bfloat16 [32, 8192, 768], P(('dp', 'ep_b', 'ep_a'))
- expert_ids: int32 [32, 8192], P(('dp', 'ep_b', 'ep_a'))
- route_order: int32 [32, 8192], P(('dp', 'ep_b', 'ep_a'))
- w_route: bfloat16 [768, 256], replicated
- expert_keys: bfloat16 [32, 256], replicated
- temperature: float32 [], replicated
- w_in: bfloat16 [32, 768, 3072], P(('ep_b', 'ep_a'))
- b_in: bfloat16 [32, 3072], P(('ep_b', 'ep_a'))
- w_out: bfloat16 [32, 3072, 768], P(('ep_b', 'ep_a'))
- b_out: bfloat16 [32, 768], P(('ep_b', 'ep_a'))
Outputs:
- output: bfloat16 [32, 8192, 768], P(('dp', 'ep_b', 'ep_a'))
All inputs are finite; a program needn't handle non-finite values.
Results may differ from the reference program's by a relative error of at most 0.00481443.
Values are sent between devices in bfloat16 or wider.
A program may use at most 768 MiB of HBM per device.

```python
import jax
import jax.numpy as jnp
from jax import lax

TOKENS_DEV = 8192
MODEL_DIM = 768
HIDDEN_DIM = 3072
ROUTER_DIM = 256
NUM_EXPERTS = 32
CAPACITY = 320
HOT_SPAN = max(1, NUM_EXPERTS // 4)


def draw_routes(route_key):
    key_list = jax.random.split(route_key, 5)
    shape_ids = (NUM_EXPERTS, TOKENS_DEV)
    spread_ids = jax.random.randint(key_list[0], shape_ids, 0, NUM_EXPERTS)
    hot_pick = jax.random.randint(key_list[1], shape_ids, 0, 4) == 0
    hot_base = jax.random.randint(key_list[2], (NUM_EXPERTS, 1), 0, NUM_EXPERTS)
    hot_ids = (hot_base + jax.random.randint(key_list[3], shape_ids, 0, HOT_SPAN)) % NUM_EXPERTS
    expert_ids = jnp.where(hot_pick, hot_ids, spread_ids).astype(jnp.int32)
    order_keys = jax.random.split(key_list[4], NUM_EXPERTS)
    route_order = jax.vmap(lambda order_key: jax.random.permutation(order_key, TOKENS_DEV))(order_keys)
    return expert_ids, route_order.astype(jnp.int32)


def setup_inputs(seed: int = 0, part: int = 0) -> dict:
    shared_keys = jax.random.split(jax.random.key(seed), 7)
    part_keys = jax.random.split(jax.random.fold_in(jax.random.key(seed + 1), part), 3)
    w_route = jax.random.normal(shared_keys[0], (MODEL_DIM, ROUTER_DIM), jnp.float32) * MODEL_DIM ** -0.5
    expert_keys = jax.random.normal(shared_keys[1], (NUM_EXPERTS, ROUTER_DIM), jnp.float32)
    temperature = jax.random.uniform(shared_keys[2], (), jnp.float32, 0.1, 0.16)
    w_in = jax.random.normal(shared_keys[3], (NUM_EXPERTS, MODEL_DIM, HIDDEN_DIM), jnp.float32) * MODEL_DIM ** -0.5
    b_in = jax.random.normal(shared_keys[4], (NUM_EXPERTS, HIDDEN_DIM), jnp.float32) * 0.5
    w_out = jax.random.normal(shared_keys[5], (NUM_EXPERTS, HIDDEN_DIM, MODEL_DIM), jnp.float32) * HIDDEN_DIM ** -0.5
    b_out = jax.random.normal(shared_keys[6], (NUM_EXPERTS, MODEL_DIM), jnp.float32) * 0.5
    expert_ids, route_order = draw_routes(part_keys[0])
    key_proj = jnp.dot(expert_keys, w_route.T)
    noise_rows = jax.random.normal(part_keys[1], (NUM_EXPERTS, TOKENS_DEV, MODEL_DIM), jnp.float32)
    strength = jax.random.uniform(part_keys[2], (NUM_EXPERTS, TOKENS_DEV, 1), jnp.float32, 0.5, 1.5)
    tokens = noise_rows + strength * key_proj[expert_ids]
    return {
        "tokens": tokens.astype(jnp.bfloat16),
        "expert_ids": expert_ids,
        "route_order": route_order,
        "w_route": w_route.astype(jnp.bfloat16),
        "expert_keys": expert_keys.astype(jnp.bfloat16),
        "temperature": temperature,
        "w_in": w_in.astype(jnp.bfloat16),
        "b_in": b_in.astype(jnp.bfloat16),
        "w_out": w_out.astype(jnp.bfloat16),
        "b_out": b_out.astype(jnp.bfloat16),
    }


def device_route(tok_rows, id_row, order_row, w_route, key_unit, temperature):
    projected = jnp.dot(tok_rows, w_route, preferred_element_type=jnp.float32)
    proj_unit = projected / jnp.sqrt(jnp.sum(projected * projected, axis=1, keepdims=True))
    router_prob = jax.nn.softmax(jnp.dot(proj_unit, key_unit.T) / temperature, axis=1)
    gate_prob = jnp.take_along_axis(router_prob, id_row[:, None], axis=1)[:, 0]
    ranked_ids = id_row[order_row]
    ranked_hot = (ranked_ids[:, None] == jnp.arange(NUM_EXPERTS)[None, :]).astype(jnp.int32)
    ranked_pos = jnp.sum(jnp.cumsum(ranked_hot, axis=0) * ranked_hot, axis=1) - 1
    slot_pos = jnp.zeros((TOKENS_DEV,), jnp.int32).at[order_row].set(ranked_pos)
    dest_slot = jnp.where(slot_pos < CAPACITY, id_row * CAPACITY + slot_pos, NUM_EXPERTS * CAPACITY)
    send_rows = jnp.zeros((NUM_EXPERTS * CAPACITY, MODEL_DIM), jnp.bfloat16).at[dest_slot].set(tok_rows, mode="drop")
    return send_rows, gate_prob, dest_slot


def expert_apply(operands):
    slot_rows, w_first, b_first, w_second, b_second = operands
    hidden = jnp.dot(slot_rows, w_first, preferred_element_type=jnp.float32) + b_first.astype(jnp.float32)
    hidden = jax.nn.gelu(hidden, approximate=False).astype(jnp.bfloat16)
    result = jnp.dot(hidden, w_second, preferred_element_type=jnp.float32) + b_second.astype(jnp.float32)
    return result.astype(jnp.bfloat16)


def reference(tokens, expert_ids, route_order, w_route, expert_keys, temperature, w_in, b_in, w_out, b_out):
    keys_f32 = expert_keys.astype(jnp.float32)
    key_unit = keys_f32 / jnp.sqrt(jnp.sum(keys_f32 * keys_f32, axis=1, keepdims=True))

    def route_one(operands):
        tok_rows, id_row, order_row = operands
        return device_route(tok_rows, id_row, order_row, w_route, key_unit, temperature)

    send_rows, gate_prob, dest_slot = lax.map(route_one, (tokens, expert_ids, route_order))
    grid_rows = send_rows.reshape(NUM_EXPERTS, NUM_EXPERTS, CAPACITY, MODEL_DIM)
    arrived = jnp.swapaxes(grid_rows, 0, 1).reshape(NUM_EXPERTS, NUM_EXPERTS * CAPACITY, MODEL_DIM)
    expert_out = lax.map(expert_apply, (arrived, w_in, b_in, w_out, b_out))
    returned = jnp.swapaxes(expert_out.reshape(NUM_EXPERTS, NUM_EXPERTS, CAPACITY, MODEL_DIM), 0, 1)
    returned = returned.reshape(NUM_EXPERTS, NUM_EXPERTS * CAPACITY, MODEL_DIM)

    def combine_one(operands):
        back_rows, dest_row, gate_row = operands
        picked = jnp.take(back_rows, dest_row, axis=0, mode="fill", fill_value=0)
        return (gate_row[:, None] * picked.astype(jnp.float32)).astype(jnp.bfloat16)

    return lax.map(combine_one, (returned, dest_slot, gate_prob))
```

```python
import functools

import jax
import jax.numpy as jnp
from jax import lax
from jax.experimental import pallas as pl
from jax.experimental.pallas import tpu as pltpu
from jax.sharding import PartitionSpec as P

EXPERT_AXES = ("ep_b", "ep_a")
MESH = pl.DeviceIdType.MESH
LANES = 128


def hot(values, size):
    return (values[:, None] == jnp.arange(size, dtype=jnp.int32)[None, :]).astype(jnp.bfloat16)


def bdot(a, b):
    return jnp.dot(a, b, preferred_element_type=jnp.float32)


def route_slots(id_row, order_row, num_experts, capacity):
    tok_dev = id_row.shape[0]
    rows = tok_dev // LANES
    slots = num_experts * capacity
    order_hi, order_lo = order_row // LANES, order_row % LANES
    hot_hi, hot_lo = hot(order_hi, rows), hot(order_lo, LANES)
    id_table = id_row.reshape(rows, LANES).astype(jnp.bfloat16)
    ranked_ids = jnp.sum(bdot(hot_hi, id_table) * hot_lo.astype(jnp.float32), axis=1).astype(jnp.int32)
    ranked_hot = hot(ranked_ids, num_experts)
    span = 256
    blocks = ranked_hot.reshape(tok_dev // span, span, num_experts)
    lower = (jnp.arange(span)[:, None] >= jnp.arange(span)[None, :]).astype(jnp.bfloat16)
    within = jnp.einsum("ij,bje->bie", lower, blocks, preferred_element_type=jnp.float32)
    totals = within[:, -1, :]
    before = jnp.cumsum(totals, axis=0) - totals
    ranked_pos = jnp.sum((within + before[:, None, :]) * blocks.astype(jnp.float32), axis=2).reshape(tok_dev)
    ranked_pos = ranked_pos.astype(jnp.int32) - 1
    ranked_slot = jnp.where(ranked_pos < capacity, ranked_ids * capacity + ranked_pos, slots)
    slot_hi, slot_lo = ranked_slot // LANES, ranked_slot % LANES
    as_col = lambda v: v.astype(jnp.bfloat16)[:, None]
    dims = (((0,), (0,)), ((), ()))
    pair = jnp.concatenate([as_col(slot_hi) * hot_lo, as_col(slot_lo) * hot_lo], axis=1)
    table = lax.dot_general(hot_hi, pair, dims, preferred_element_type=jnp.float32).astype(jnp.int32)
    dest_slot = (table[:, :LANES] * LANES + table[:, LANES:]).reshape(tok_dev)
    shot_hi, shot_lo = hot(slot_hi, slots // LANES), hot(slot_lo, LANES)
    pair = jnp.concatenate([as_col(order_hi) * shot_lo, as_col(order_lo) * shot_lo], axis=1)
    table = lax.dot_general(shot_hi, pair, dims, preferred_element_type=jnp.float32).astype(jnp.int32)
    slot_source = (table[:, :LANES] * LANES + table[:, LANES:]).reshape(slots)
    return slot_source, dest_slot


def gates(tok_rows, id_row, w_route, expert_keys, tau):
    num_experts = expert_keys.shape[0]
    keys_f32 = expert_keys.astype(jnp.float32)
    key_unit = keys_f32 / jnp.sqrt(jnp.sum(keys_f32 * keys_f32, axis=1, keepdims=True))
    projected = jnp.dot(tok_rows, w_route, preferred_element_type=jnp.float32)
    proj_unit = projected / jnp.sqrt(jnp.sum(projected * projected, axis=1, keepdims=True))
    router_prob = jax.nn.softmax(jnp.dot(proj_unit, key_unit.T) / tau, axis=1)
    expert_range = jnp.arange(num_experts, dtype=jnp.int32)[None, :]
    return jnp.sum(jnp.where(id_row[:, None] == expert_range, router_prob, 0.0), axis=1)


def send_order(nb, nx):
    rest = [(y, x) for y in range(nb) for x in range(nx) if (y, x) != (0, 0)]

    def phase(off):
        y, x = off
        near = lambda v, n: v in (1, n - 1)
        if x == 0 or y == 0:
            return 0 if near(x, nx) or near(y, nb) else 3
        if near(x, nx) and near(y, nb):
            return 1 if (x == 1) == (y == 1) else 2
        return 4 if not near(x, nx) and not near(y, nb) else 5

    rest.sort(key=phase)
    out = [(0, 0, 0), (0, 0, 1)]
    for p in range(6):
        out += [(y, x, c) for c in range(2) for (y, x) in rest if phase((y, x)) == p]
    return out


def exchange_kernel(order, nb, nx, s_ref, w1_hbm, b1_ref, w2_hbm, b2_ref, r_ref,
                    a_buf, h_buf, w1_v, w2_v, wsem, lsem, send1, recv1, send2, recv2):
    count = len(order)
    row_b, row_a = lax.axis_index("ep_b"), lax.axis_index("ep_a")
    row_x, row_c = row_a // 2, lax.rem(row_a, 2)
    me = row_b * (2 * nx) + row_a
    w1_copy = pltpu.make_async_copy(w1_hbm, w1_v, wsem.at[0])
    w2_copy = pltpu.make_async_copy(w2_hbm, w2_v, wsem.at[1])
    own_in = pltpu.make_async_copy(s_ref.at[me], a_buf.at[0], lsem.at[0])
    w1_copy.start()
    w2_copy.start()
    own_in.start()

    def peer(y, x, c):
        return lax.rem(row_b + y, nb), lax.rem(row_x + x, nx) * 2 + lax.rem(row_c + c, 2)

    barrier = pltpu.get_barrier_semaphore()
    for y, x, c in order[1:]:
        pb, pa = peer(y, x, c)
        pl.semaphore_signal(barrier, inc=1, device_id={"ep_b": pb, "ep_a": pa}, device_id_type=MESH)
    pl.semaphore_wait(barrier, count - 1)

    out_copies = []
    for k in range(1, count):
        pb, pa = peer(*order[k])
        copy = pltpu.make_async_remote_copy(
            src_ref=s_ref.at[pb * (2 * nx) + pa], dst_ref=a_buf.at[k], send_sem=send1.at[k], recv_sem=recv1.at[k],
            device_id={"ep_b": pb, "ep_a": pa}, device_id_type=MESH)
        copy.start()
        out_copies.append(copy)

    words = []
    for w in range(0, count, 5):
        word = 0
        for j, (y, x, c) in enumerate(order[w:w + 5]):
            word += (((-y) % nb) * (2 * nx) + ((-x) % nx) * 2 + c) << (6 * j)
        words.append(word)

    def back_copy(k):
        word = 0
        for w, value in enumerate(words):
            word = word + jnp.where(k // 5 == w, value, 0)
        code = lax.rem(lax.shift_right_logical(word, 6 * lax.rem(k, 5)), 64)
        pb, pa = peer(code // (2 * nx), lax.rem(code // 2, nx), lax.rem(code, 2))
        return pltpu.make_async_remote_copy(
            src_ref=a_buf.at[k], dst_ref=r_ref.at[me], send_sem=send2.at[k], recv_sem=recv2.at[k],
            device_id={"ep_b": pb, "ep_a": pa}, device_id_type=MESH)

    rows = 2 * a_buf.shape[1]
    hidden, width = w1_v.shape[1], w1_v.shape[0]
    n1, n2 = 512, 256

    def mlp(pair):
        x = a_buf[pl.ds(pair * 2, 2)].reshape(rows, width)
        for n in range(0, hidden, n1):
            part = jnp.dot(x, w1_v[:, n:n + n1], preferred_element_type=jnp.float32) + b1_ref[:, n:n + n1]
            part = 0.5 * part * (1.0 + lax.erf(part * 0.7071067811865476))
            h_buf[:, n:n + n1] = part.astype(jnp.bfloat16)
        for n in range(0, width, n2):
            y = jnp.dot(h_buf[...], w2_v[:, n:n + n2], preferred_element_type=jnp.float32) + b2_ref[:, n:n + n2]
            a_buf[pl.ds(pair * 2, 2), :, n:n + n2] = y.astype(jnp.bfloat16).reshape(2, rows // 2, n2)

    own_in.wait()
    w1_copy.wait()
    w2_copy.wait()
    out_copies[0].wait_recv()
    mlp(0)
    own_out = pltpu.make_async_copy(a_buf.at[0], r_ref.at[me], lsem.at[1])
    own_out.start()
    back_copy(1).start()

    near_b, near_a = peer(*order[1])

    def arrived(k):
        pltpu.make_async_remote_copy(
            src_ref=s_ref.at[me], dst_ref=a_buf.at[k], send_sem=send1.at[k], recv_sem=recv1.at[k],
            device_id={"ep_b": near_b, "ep_a": near_a}, device_id_type=MESH).wait_recv()

    def loop_step(pair, carry):
        arrived(2 * pair)
        arrived(2 * pair + 1)
        mlp(pair)
        back_copy(2 * pair).start()
        back_copy(2 * pair + 1).start()
        return carry

    lax.fori_loop(1, count // 2, loop_step, 0)
    own_out.wait()
    for copy in out_copies:
        copy.wait_send()

    def drain(k, carry):
        copy = back_copy(k)
        copy.wait_send()
        copy.wait_recv()
        return carry

    lax.fori_loop(1, count, drain, 0)


def exchange(send_rows, w_first, b_first, w_second, b_second, nb, na):
    count, capacity, width = send_rows.shape
    hidden = w_first.shape[1]
    nx = na // 2
    order = send_order(nb, nx)
    any_spec = pl.BlockSpec(memory_space=pl.ANY)
    vmem_spec = pl.BlockSpec(memory_space=pltpu.VMEM)
    flops = 4 * count * capacity * width * hidden
    return pl.pallas_call(
        functools.partial(exchange_kernel, order, nb, nx),
        name="exchange_mlp",
        out_shape=jax.ShapeDtypeStruct((count, capacity, width), jnp.bfloat16),
        in_specs=[any_spec, any_spec, vmem_spec, any_spec, vmem_spec],
        out_specs=any_spec,
        scratch_shapes=[
            pltpu.VMEM((count, capacity, width), jnp.bfloat16),
            pltpu.VMEM((2 * capacity, hidden), jnp.bfloat16),
            pltpu.VMEM((width, hidden), jnp.bfloat16),
            pltpu.VMEM((hidden, width), jnp.bfloat16),
            pltpu.SemaphoreType.DMA((2,)),
            pltpu.SemaphoreType.DMA((2,)),
            pltpu.SemaphoreType.DMA((count,)),
            pltpu.SemaphoreType.DMA((count,)),
            pltpu.SemaphoreType.DMA((count,)),
            pltpu.SemaphoreType.DMA((count,)),
        ],
        cost_estimate=pl.CostEstimate(flops=flops, bytes_accessed=4 * count * capacity * width, transcendentals=0),
        compiler_params=pltpu.CompilerParams(
            collective_id=0, has_side_effects=True, vmem_limit_bytes=60 * 1024 * 1024),
    )(send_rows, w_first, b_first.astype(jnp.float32)[None], w_second, b_second.astype(jnp.float32)[None])


def combine_local(back_rows, dest_slot, gate_prob):
    picked = jnp.take(back_rows, dest_slot, axis=0, mode="fill", fill_value=0)
    return (gate_prob[:, None] * picked.astype(jnp.float32)).astype(jnp.bfloat16)


def solution(mesh):
    nb, na = mesh.shape["ep_b"], mesh.shape["ep_a"]
    num_experts = nb * na
    tok_spec = P(("dp",) + EXPERT_AXES)
    expert_spec = P(EXPERT_AXES)

    def device_step(tokens, expert_ids, route_order, w_route, expert_keys, tau, w_in, b_in, w_out, b_out):
        tok_dev, model_width = tokens.shape[1], tokens.shape[2]
        capacity = (5 * tok_dev + 4 * num_experts - 1) // (4 * num_experts)
        slot_source, dest_slot = route_slots(expert_ids[0], route_order[0], num_experts, capacity)
        send_rows = jnp.take(tokens[0], slot_source, axis=0, mode="clip").reshape(num_experts, capacity, model_width)
        gate_prob = gates(tokens[0], expert_ids[0], w_route, expert_keys, tau)
        returned = exchange(send_rows, w_in[0], b_in[0], w_out[0], b_out[0], nb, na)
        return combine_local(returned.reshape(num_experts * capacity, model_width), dest_slot, gate_prob)[None]

    return jax.shard_map(
        device_step,
        mesh=mesh,
        in_specs=(tok_spec, tok_spec, tok_spec, P(), P(), P(), expert_spec, expert_spec, expert_spec, expert_spec),
        out_specs=tok_spec,
        check_vma=False,
    )
```

```python
import functools

import jax
import jax.numpy as jnp
from jax import lax
from jax.experimental import pallas as pl
from jax.experimental.pallas import tpu as pltpu
from jax.sharding import PartitionSpec as P

EXPERT_AXES = ("ep_b", "ep_a")
MESH = pl.DeviceIdType.MESH
LANES = 128


def hot(values, size):
    return (values[:, None] == jnp.arange(size, dtype=jnp.int32)[None, :]).astype(jnp.bfloat16)


def bdot(a, b):
    return jnp.dot(a, b, preferred_element_type=jnp.float32)


def route_slots(id_row, order_row, num_experts, capacity):
    tok_dev = id_row.shape[0]
    rows = tok_dev // LANES
    slots = num_experts * capacity
    order_hi, order_lo = order_row // LANES, order_row % LANES
    hot_hi, hot_lo = hot(order_hi, rows), hot(order_lo, LANES)
    id_table = id_row.reshape(rows, LANES).astype(jnp.bfloat16)
    ranked_ids = jnp.sum(bdot(hot_hi, id_table) * hot_lo.astype(jnp.float32), axis=1).astype(jnp.int32)
    ranked_hot = hot(ranked_ids, num_experts)
    span = 256
    blocks = ranked_hot.reshape(tok_dev // span, span, num_experts)
    lower = (jnp.arange(span)[:, None] >= jnp.arange(span)[None, :]).astype(jnp.bfloat16)
    within = jnp.einsum("ij,bje->bie", lower, blocks, preferred_element_type=jnp.float32)
    totals = within[:, -1, :]
    before = jnp.cumsum(totals, axis=0) - totals
    ranked_pos = jnp.sum((within + before[:, None, :]) * blocks.astype(jnp.float32), axis=2).reshape(tok_dev)
    ranked_pos = ranked_pos.astype(jnp.int32) - 1
    ranked_slot = jnp.where(ranked_pos < capacity, ranked_ids * capacity + ranked_pos, slots)
    slot_hi, slot_lo = ranked_slot // LANES, ranked_slot % LANES
    as_col = lambda v: v.astype(jnp.bfloat16)[:, None]
    dims = (((0,), (0,)), ((), ()))
    pair = jnp.concatenate([as_col(slot_hi) * hot_lo, as_col(slot_lo) * hot_lo], axis=1)
    table = lax.dot_general(hot_hi, pair, dims, preferred_element_type=jnp.float32).astype(jnp.int32)
    dest_slot = (table[:, :LANES] * LANES + table[:, LANES:]).reshape(tok_dev)
    shot_hi, shot_lo = hot(slot_hi, slots // LANES), hot(slot_lo, LANES)
    pair = jnp.concatenate([as_col(order_hi) * shot_lo, as_col(order_lo) * shot_lo], axis=1)
    table = lax.dot_general(shot_hi, pair, dims, preferred_element_type=jnp.float32).astype(jnp.int32)
    slot_source = (table[:, :LANES] * LANES + table[:, LANES:]).reshape(slots)
    return slot_source, dest_slot


def send_order(nb, nx):
    rest = [(y, x) for y in range(nb) for x in range(nx) if (y, x) != (0, 0)]

    def phase(off):
        y, x = off
        near = lambda v, n: v in (1, n - 1)
        if x == 0 or y == 0:
            return 0 if near(x, nx) or near(y, nb) else 3
        if near(x, nx) and near(y, nb):
            return 1 if (x == 1) == (y == 1) else 2
        return 4 if not near(x, nx) and not near(y, nb) else 5

    rest.sort(key=phase)
    out = [(0, 0, 0), (0, 0, 1)]
    for p in range(6):
        out += [(y, x, c) for c in range(2) for (y, x) in rest if phase((y, x)) == p]
    return out


def exchange_kernel(order, nb, nx, source_ref, ids_ref, tau_ref, tok_hbm, wr_ref, key_ref, w1_hbm, b1_ref, w2_hbm, b2_ref,
                    r_ref, s_ref, gate_ref, wide, a_buf, h_buf, w1_v, w2_v, gathered, stage,
                    wsem, lsem, tsem, gsem, send1, recv1, send2, recv2):
    count, capacity, width = a_buf.shape
    hidden = w1_v.shape[1]
    tok_dev = tok_hbm.shape[0]
    parts = width // LANES
    row_b, row_a = lax.axis_index("ep_b"), lax.axis_index("ep_a")
    row_x, row_c = row_a // 2, lax.rem(row_a, 2)
    me = row_b * (2 * nx) + row_a

    def peer(y, x, c):
        return lax.rem(row_b + y, nb), lax.rem(row_x + x, nx) * 2 + lax.rem(row_c + c, 2)

    barrier = pltpu.get_barrier_semaphore()
    for y, x, c in order[1:]:
        pb, pa = peer(y, x, c)
        pl.semaphore_signal(barrier, inc=1, device_id={"ep_b": pb, "ep_a": pa}, device_id_type=MESH)

    chunk, depth = 512, h_buf.shape[0]
    chunks = tok_dev // chunk

    def token_load(i):
        slot = lax.rem(i, depth)
        return pltpu.make_async_copy(
            tok_hbm.at[pl.ds(pl.multiple_of(i * chunk, chunk), chunk)], h_buf.at[slot, pl.ds(0, chunk)], tsem.at[slot])

    for i in range(depth - 1):
        token_load(i).start()

    def widen(i, carry):
        @pl.when(i + depth - 1 < chunks)
        def _():
            token_load(i + depth - 1).start()
        token_load(i).wait()
        for j in range(parts):
            piece = h_buf[lax.rem(i, depth), pl.ds(0, chunk), j * LANES:(j + 1) * LANES].astype(jnp.float32)
            wide[pl.ds(i * chunk * parts + j, chunk, stride=parts), :] = piece
        return carry

    lax.fori_loop(0, chunks, widen, 0)
    w1_copy = pltpu.make_async_copy(w1_hbm, w1_v, wsem.at[0])
    w2_copy = pltpu.make_async_copy(w2_hbm, w2_v, wsem.at[1])
    w1_copy.start()
    w2_copy.start()

    words = []
    for w in range(0, count, 5):
        word = 0
        for j, (y, x, c) in enumerate(order[w:w + 5]):
            word += (y * (2 * nx) + x * 2 + c) << (6 * j)
        words.append(word)

    def offset(k):
        word = 0
        for w, value in enumerate(words):
            word = word + jnp.where(k // 5 == w, value, 0)
        code = lax.rem(lax.shift_right_logical(word, 6 * lax.rem(k, 5)), 64)
        return code // (2 * nx), lax.rem(code // 2, nx), lax.rem(code, 2)

    def fill(block, slot):
        def rows16(r, carry):
            for q in range(16):
                src = source_ref[block * capacity + r * 16 + q]
                gathered[pl.ds((r * 16 + q) * parts, parts), :] = wide[pl.ds(src * parts, parts), :]
            return carry
        lax.fori_loop(0, capacity // 16, rows16, 0)
        for j in range(parts):
            stage[slot, :, j * LANES:(j + 1) * LANES] = gathered[pl.ds(j, capacity, stride=parts), :].astype(jnp.bfloat16)

    def stage_copy(k, slot):
        y, x, c = offset(k)
        pb, pa = peer(y, x, c)
        return pltpu.make_async_copy(stage.at[slot], s_ref.at[pb * (2 * nx) + pa], gsem.at[slot])

    def send_copy(k):
        y, x, c = offset(k)
        pb, pa = peer(y, x, c)
        return pltpu.make_async_remote_copy(
            src_ref=s_ref.at[pb * (2 * nx) + pa], dst_ref=a_buf.at[k], send_sem=send1.at[k], recv_sem=recv1.at[k],
            device_id={"ep_b": pb, "ep_a": pa}, device_id_type=MESH)

    def back_copy(k):
        y, x, c = offset(k)
        pb, pa = peer(nb - y, nx - x, c)
        return pltpu.make_async_remote_copy(
            src_ref=a_buf.at[k], dst_ref=r_ref.at[me], send_sem=send2.at[k], recv_sem=recv2.at[k],
            device_id={"ep_b": pb, "ep_a": pa}, device_id_type=MESH)

    pl.semaphore_wait(barrier, count - 1)

    def fill_step(k, carry):
        y, x, c = offset(k)
        pb, pa = peer(y, x, c)
        slot = lax.rem(k, 2)
        fill(pb * (2 * nx) + pa, slot)
        stage_copy(k, slot).start()

        @pl.when(k > 1)
        def _():
            stage_copy(k - 1, 1 - slot).wait()
            send_copy(k - 1).start()
        return carry

    lax.fori_loop(1, count, fill_step, 0)
    stage_copy(count - 1, (count - 1) % 2).wait()
    send_copy(count - 1).start()
    fill(me, 0)
    own_in = pltpu.make_async_copy(stage.at[0], s_ref.at[me], lsem.at[0])
    own_in.start()
    own_in.wait()
    own_in = pltpu.make_async_copy(s_ref.at[me], a_buf.at[0], lsem.at[0])
    own_in.start()

    rows = 2 * capacity
    n1, n2 = 384, 256
    per = width // n1

    def mlp(pair):
        x = a_buf[pl.ds(pair * 2, 2)].reshape(rows, width)
        for n in range(hidden // n1):
            cols = pl.ds(n * n1, n1)
            part = jnp.dot(x, w1_v[:, cols], preferred_element_type=jnp.float32) + b1_ref[:, cols]
            part = 0.5 * part * (1.0 + lax.erf(part * 0.7071067811865476))
            h_buf[n // per, :, (n % per) * n1:(n % per + 1) * n1] = part.astype(jnp.bfloat16)
        for n in range(0, width, n2):
            h = jnp.concatenate([h_buf[q] for q in range(depth)], axis=1)
            y = jnp.dot(h, w2_v[:, n:n + n2], preferred_element_type=jnp.float32) + b2_ref[:, n:n + n2]
            a_buf[pl.ds(pair * 2, 2), :, n:n + n2] = y.astype(jnp.bfloat16).reshape(2, capacity, n2)

    own_in.wait()
    w1_copy.wait()
    w2_copy.wait()

    def loop_step(pair, carry):
        @pl.when(pair > 0)
        def _():
            send_copy(2 * pair).wait_recv()
        send_copy(2 * pair + 1).wait_recv()
        mlp(pair)

        @pl.when(pair > 0)
        def _():
            back_copy(2 * pair).start()
        back_copy(2 * pair + 1).start()
        return carry

    lax.fori_loop(0, count // 2, loop_step, 0)
    own_out = pltpu.make_async_copy(a_buf.at[0], r_ref.at[me], lsem.at[1])
    own_out.start()

    key = key_ref[...].astype(jnp.float32)
    key_unit = key / jnp.sqrt(jnp.sum(key * key, axis=1, keepdims=True))
    for i in range(depth - 1):
        token_load(i).start()

    def gate_step(i, carry):
        @pl.when(i + depth - 1 < chunks)
        def _():
            token_load(i + depth - 1).start()
        token_load(i).wait()
        x = h_buf[lax.rem(i, depth), pl.ds(0, chunk), :]
        proj = lax.dot_general(wr_ref[...], x, (((1,), (1,)), ((), ())), preferred_element_type=jnp.float32)
        unit = proj / jnp.sqrt(jnp.sum(proj * proj, axis=0, keepdims=True))
        logits = jnp.dot(key_unit, unit, precision=lax.Precision.HIGHEST, preferred_element_type=jnp.float32) / tau_ref[0, 0]
        weight = jnp.exp(logits - jnp.max(logits, axis=0, keepdims=True))
        cols = pl.ds(pl.multiple_of(i * chunk, chunk), chunk)
        expert = lax.broadcasted_iota(jnp.int32, weight.shape, 0)
        mine = jnp.sum(jnp.where(expert == ids_ref[:, cols], weight, 0.0), axis=0, keepdims=True)
        gate_ref[:, cols] = mine / jnp.sum(weight, axis=0, keepdims=True)
        return carry

    lax.fori_loop(0, chunks, gate_step, 0)
    own_out.wait()

    def drain(k, carry):
        send_copy(k).wait_send()
        copy = back_copy(k)
        copy.wait_send()
        copy.wait_recv()
        return carry

    lax.fori_loop(1, count, drain, 0)


def exchange(tokens, id_row, slot_source, w_route, expert_keys, tau, w_first, b_first, w_second, b_second, nb, na):
    tok_dev, width = tokens.shape
    count = nb * na
    capacity = slot_source.shape[0] // count
    hidden = w_first.shape[1]
    nx = na // 2
    order = send_order(nb, nx)
    any_spec = pl.BlockSpec(memory_space=pl.ANY)
    vmem_spec = pl.BlockSpec(memory_space=pltpu.VMEM)
    smem_spec = pl.BlockSpec(memory_space=pltpu.SMEM)
    flops = 4 * count * capacity * width * hidden
    blocks = jax.ShapeDtypeStruct((count, capacity, width), jnp.bfloat16)
    dma = lambda n: pltpu.SemaphoreType.DMA((n,))
    returned, _, gate = pl.pallas_call(
        functools.partial(exchange_kernel, order, nb, nx),
        name="exchange_mlp",
        out_shape=(blocks, blocks, jax.ShapeDtypeStruct((1, tok_dev), jnp.float32)),
        in_specs=[smem_spec, vmem_spec, smem_spec, any_spec, vmem_spec, vmem_spec, any_spec, vmem_spec, any_spec, vmem_spec],
        out_specs=(any_spec, any_spec, vmem_spec),
        scratch_shapes=[
            pltpu.VMEM((tok_dev * (width // LANES), LANES), jnp.float32),
            pltpu.VMEM((count, capacity, width), jnp.bfloat16),
            pltpu.VMEM((hidden // width, 2 * capacity, width), jnp.bfloat16),
            pltpu.VMEM((width, hidden), jnp.bfloat16),
            pltpu.VMEM((hidden, width), jnp.bfloat16),
            pltpu.VMEM((capacity * (width // LANES), LANES), jnp.float32),
            pltpu.VMEM((2, capacity, width), jnp.bfloat16),
            dma(2), dma(2), dma(hidden // width), dma(2), dma(count), dma(count), dma(count), dma(count),
        ],
        cost_estimate=pl.CostEstimate(flops=flops, bytes_accessed=6 * count * capacity * width, transcendentals=0),
        compiler_params=pltpu.CompilerParams(
            collective_id=0, has_side_effects=True, vmem_limit_bytes=67000000),
    )(slot_source, id_row[None], tau.reshape(1, 1), tokens, w_route.T, expert_keys,
      w_first, b_first.astype(jnp.float32)[None], w_second, b_second.astype(jnp.float32)[None])
    return returned.reshape(count * capacity, width), gate.reshape(tok_dev)


def combine_kernel(dest_ref, gate_ref, back_ref, out_ref, wide, gathered, in_buf, out_buf, in_sem, out_sem):
    slots, width = back_ref.shape
    tokens = out_ref.shape[0]
    parts = width // LANES
    rows = in_buf.shape[1]
    depth = in_buf.shape[0]
    loads = slots // rows

    def load(i):
        return pltpu.make_async_copy(back_ref.at[pl.ds(pl.multiple_of(i * rows, rows), rows)], in_buf.at[lax.rem(i, depth)], in_sem.at[lax.rem(i, depth)])

    for i in range(depth - 1):
        load(i).start()
    wide[pl.ds(slots * parts, 8), :] = jnp.zeros((8, LANES), jnp.float32)

    def widen(i, carry):
        @pl.when(i + depth - 1 < loads)
        def _():
            load(i + depth - 1).start()
        load(i).wait()
        for j in range(parts):
            piece = in_buf[lax.rem(i, depth), :, j * LANES:(j + 1) * LANES].astype(jnp.float32)
            wide[pl.ds(i * rows * parts + j, rows, stride=parts), :] = piece
        return carry

    lax.fori_loop(0, loads, widen, 0)

    def store(i):
        return pltpu.make_async_copy(out_buf.at[lax.rem(i, 2)], out_ref.at[pl.ds(pl.multiple_of(i * rows, rows), rows)], out_sem.at[lax.rem(i, 2)])

    def gather(i, carry):
        def row(r, c):
            base = r * 16
            for q in range(16):
                t = i * rows + base + q
                gathered[pl.ds((base + q) * parts, parts), :] = wide[pl.ds(dest_ref[t] * parts, parts), :] * gate_ref[t]
            return c
        lax.fori_loop(0, rows // 16, row, 0)
        @pl.when(i >= 2)
        def _():
            store(i - 2).wait()
        for j in range(parts):
            out_buf[lax.rem(i, 2), :, j * LANES:(j + 1) * LANES] = gathered[pl.ds(j, rows, stride=parts), :].astype(jnp.bfloat16)
        store(i).start()
        return carry

    lax.fori_loop(0, tokens // rows, gather, 0)
    store(tokens // rows - 2).wait()
    store(tokens // rows - 1).wait()

def combine(back, dest, gate):
    slots, width = back.shape
    tokens = dest.shape[0]
    parts = width // LANES
    rows = 512
    smem = pl.BlockSpec(memory_space=pltpu.SMEM)
    hbm = pl.BlockSpec(memory_space=pl.ANY)
    return pl.pallas_call(combine_kernel, name="combine",
        out_shape=jax.ShapeDtypeStruct((tokens, width), jnp.bfloat16),
        in_specs=[smem, smem, hbm], out_specs=hbm,
        scratch_shapes=[pltpu.VMEM((slots * parts + 8, LANES), jnp.float32), pltpu.VMEM((rows * parts, LANES), jnp.float32),
            pltpu.VMEM((4, rows, width), jnp.bfloat16), pltpu.VMEM((2, rows, width), jnp.bfloat16),
            pltpu.SemaphoreType.DMA((4,)), pltpu.SemaphoreType.DMA((2,))],
        compiler_params=pltpu.CompilerParams(vmem_limit_bytes=60 * 1024 * 1024))(dest, gate, back)


def solution(mesh):
    nb, na = mesh.shape["ep_b"], mesh.shape["ep_a"]
    num_experts = nb * na
    tok_spec = P(("dp",) + EXPERT_AXES)
    expert_spec = P(EXPERT_AXES)

    def device_step(tokens, expert_ids, route_order, w_route, expert_keys, tau, w_in, b_in, w_out, b_out):
        tok_dev, model_width = tokens.shape[1], tokens.shape[2]
        capacity = (5 * tok_dev + 4 * num_experts - 1) // (4 * num_experts)
        slot_source, dest_slot = route_slots(expert_ids[0], route_order[0], num_experts, capacity)
        returned, gate = exchange(tokens[0], expert_ids[0], slot_source, w_route, expert_keys, tau,
                                  w_in[0], b_in[0], w_out[0], b_out[0], nb, na)
        return combine(returned, dest_slot, gate)[None]

    return jax.shard_map(
        device_step,
        mesh=mesh,
        in_specs=(tok_spec, tok_spec, tok_spec, P(), P(), P(), expert_spec, expert_spec, expert_spec, expert_spec),
        out_specs=tok_spec,
        check_vma=False,
    )
```

```python
import functools

import jax
import jax.numpy as jnp
from jax import lax
from jax.experimental import pallas as pl
from jax.experimental.pallas import tpu as pltpu
from jax.sharding import PartitionSpec as P

EXPERT_AXES = ("ep_b", "ep_a")
MESH = pl.DeviceIdType.MESH
LANES = 128


def hot(values, size):
    return (values[:, None] == jnp.arange(size, dtype=jnp.int32)[None, :]).astype(jnp.bfloat16)


def bdot(a, b):
    return jnp.dot(a, b, preferred_element_type=jnp.float32)


def route_slots(id_row, order_row, num_experts, capacity):
    tok_dev = id_row.shape[0]
    rows = tok_dev // LANES
    slots = num_experts * capacity
    order_hi, order_lo = order_row // LANES, order_row % LANES
    hot_hi, hot_lo = hot(order_hi, rows), hot(order_lo, LANES)
    id_table = id_row.reshape(rows, LANES).astype(jnp.bfloat16)
    ranked_ids = jnp.sum(bdot(hot_hi, id_table) * hot_lo.astype(jnp.float32), axis=1).astype(jnp.int32)
    ranked_hot = hot(ranked_ids, num_experts)
    span = 256
    blocks = ranked_hot.reshape(tok_dev // span, span, num_experts)
    lower = (jnp.arange(span)[:, None] >= jnp.arange(span)[None, :]).astype(jnp.bfloat16)
    within = jnp.einsum("ij,bje->bie", lower, blocks, preferred_element_type=jnp.float32)
    totals = within[:, -1, :]
    before = jnp.cumsum(totals, axis=0) - totals
    ranked_pos = jnp.sum((within + before[:, None, :]) * blocks.astype(jnp.float32), axis=2).reshape(tok_dev)
    ranked_pos = ranked_pos.astype(jnp.int32) - 1
    ranked_slot = jnp.where(ranked_pos < capacity, ranked_ids * capacity + ranked_pos, slots)
    slot_hi, slot_lo = ranked_slot // LANES, ranked_slot % LANES
    as_col = lambda v: v.astype(jnp.bfloat16)[:, None]
    dims = (((0,), (0,)), ((), ()))
    pair = jnp.concatenate([as_col(slot_hi) * hot_lo, as_col(slot_lo) * hot_lo], axis=1)
    table = lax.dot_general(hot_hi, pair, dims, preferred_element_type=jnp.float32).astype(jnp.int32)
    dest_slot = (table[:, :LANES] * LANES + table[:, LANES:]).reshape(tok_dev)
    shot_hi, shot_lo = hot(slot_hi, slots // LANES), hot(slot_lo, LANES)
    pair = jnp.concatenate([as_col(order_hi) * shot_lo, as_col(order_lo) * shot_lo], axis=1)
    table = lax.dot_general(shot_hi, pair, dims, preferred_element_type=jnp.float32).astype(jnp.int32)
    slot_source = (table[:, :LANES] * LANES + table[:, LANES:]).reshape(slots)
    return slot_source, dest_slot


def send_order(nb, nx):
    near = lambda y, x: [(y, x), ((nb - y) % nb, (nx - x) % nx)]
    pair = lambda offs, c: [(y, x, c) for y, x in offs]
    far = lambda y, x: [(y, x, 0), (y, x, 1)]
    hy, hx = nb // 2, nx // 2
    col, row = near(1, 0), near(0, 1)
    same, cross = near(1, 1), near(1, nx - 1)
    x_one, y_one = near(hy, 1), near(1, hx)
    return ([(0, 0, 0), (0, 0, 1)] + pair(col, 0) + pair(same, 0) + pair(col, 1) + pair(same, 1) + far(hy, 0)
            + pair(cross, 0) + pair(cross, 1) + pair(x_one, 0) + pair(row, 0) + pair(x_one, 1) + pair(row, 1)
            + far(0, hx) + pair(y_one, 0) + pair(y_one, 1) + far(hy, hx))


def exchange_kernel(order, nb, nx, source_ref, ids_ref, tau_ref, tok_hbm, wr_ref, key_ref, w1_hbm, b1_ref, w2_hbm, b2_ref,
                    r_ref, s_ref, gate_ref, wide, a_buf, h_buf, w1_v, w2_v, gathered, stage,
                    wsem, lsem, tsem, gsem, send1, recv1, send2, recv2):
    count, capacity, width = a_buf.shape
    hidden = w1_v.shape[1]
    tok_dev = tok_hbm.shape[0]
    parts = width // LANES
    row_b, row_a = lax.axis_index("ep_b"), lax.axis_index("ep_a")
    row_x, row_c = row_a // 2, lax.rem(row_a, 2)
    me = row_b * (2 * nx) + row_a

    def peer(y, x, c):
        return lax.rem(row_b + y, nb), lax.rem(row_x + x, nx) * 2 + lax.rem(row_c + c, 2)

    barrier = pltpu.get_barrier_semaphore()
    for y, x, c in order[1:]:
        pb, pa = peer(y, x, c)
        pl.semaphore_signal(barrier, inc=1, device_id={"ep_b": pb, "ep_a": pa}, device_id_type=MESH)

    chunk, depth = 512, h_buf.shape[0]
    chunks = tok_dev // chunk

    def token_load(i):
        slot = lax.rem(i, depth)
        return pltpu.make_async_copy(
            tok_hbm.at[pl.ds(pl.multiple_of(i * chunk, chunk), chunk)], h_buf.at[slot, pl.ds(0, chunk)], tsem.at[slot])

    for i in range(depth - 1):
        token_load(i).start()

    def widen(i, carry):
        @pl.when(i + depth - 1 < chunks)
        def _():
            token_load(i + depth - 1).start()
        token_load(i).wait()
        for j in range(parts):
            piece = h_buf[lax.rem(i, depth), pl.ds(0, chunk), j * LANES:(j + 1) * LANES].astype(jnp.float32)
            wide[pl.ds(i * chunk * parts + j, chunk, stride=parts), :] = piece
        return carry

    lax.fori_loop(0, chunks, widen, 0)
    w1_copy = pltpu.make_async_copy(w1_hbm, w1_v, wsem.at[0])
    w2_copy = pltpu.make_async_copy(w2_hbm, w2_v, wsem.at[1])
    w1_copy.start()
    w2_copy.start()

    words = []
    for w in range(0, count, 5):
        word = 0
        for j, (y, x, c) in enumerate(order[w:w + 5]):
            word += (y * (2 * nx) + x * 2 + c) << (6 * j)
        words.append(word)

    def offset(k):
        word = 0
        for w, value in enumerate(words):
            word = word + jnp.where(k // 5 == w, value, 0)
        code = lax.rem(lax.shift_right_logical(word, 6 * lax.rem(k, 5)), 64)
        return code // (2 * nx), lax.rem(code // 2, nx), lax.rem(code, 2)

    def fill(block, slot):
        def rows16(r, carry):
            for q in range(16):
                src = source_ref[block * capacity + r * 16 + q]
                gathered[pl.ds((r * 16 + q) * parts, parts), :] = wide[pl.ds(src * parts, parts), :]
            return carry
        lax.fori_loop(0, capacity // 16, rows16, 0)
        for j in range(parts):
            stage[slot, :, j * LANES:(j + 1) * LANES] = gathered[pl.ds(j, capacity, stride=parts), :].astype(jnp.bfloat16)

    def stage_copy(k, slot):
        y, x, c = offset(k)
        pb, pa = peer(y, x, c)
        return pltpu.make_async_copy(stage.at[slot], s_ref.at[pb * (2 * nx) + pa], gsem.at[slot])

    def send_copy(k):
        y, x, c = offset(k)
        pb, pa = peer(y, x, c)
        return pltpu.make_async_remote_copy(
            src_ref=s_ref.at[pb * (2 * nx) + pa], dst_ref=a_buf.at[k], send_sem=send1.at[k], recv_sem=recv1.at[k],
            device_id={"ep_b": pb, "ep_a": pa}, device_id_type=MESH)

    def back_copy(k):
        y, x, c = offset(k)
        pb, pa = peer(nb - y, nx - x, c)
        return pltpu.make_async_remote_copy(
            src_ref=a_buf.at[k], dst_ref=r_ref.at[me], send_sem=send2.at[k], recv_sem=recv2.at[k],
            device_id={"ep_b": pb, "ep_a": pa}, device_id_type=MESH)

    def turn(step):
        return step + jnp.where((step // 4) == 2, row_c * (1 - 2 * lax.rem(step, 2)), 0)

    def seq(i):
        return jnp.where(i < 2, i, 2 * turn(i // 2) + lax.rem(i + row_c, 2))

    pl.semaphore_wait(barrier, count - 1)

    def fill_step(i, carry):
        k = seq(i)
        y, x, c = offset(k)
        pb, pa = peer(y, x, c)
        slot = lax.rem(i, 2)
        fill(pb * (2 * nx) + pa, slot)
        stage_copy(k, slot).start()

        @pl.when(i > 1)
        def _():
            before = seq(i - 1)
            stage_copy(before, 1 - slot).wait()
            send_copy(before).start()
        return carry

    lax.fori_loop(1, count, fill_step, 0)
    last = seq(count - 1)
    stage_copy(last, (count - 1) % 2).wait()
    send_copy(last).start()
    fill(me, 0)
    own_in = pltpu.make_async_copy(stage.at[0], s_ref.at[me], lsem.at[0])
    own_in.start()
    own_in.wait()
    own_in = pltpu.make_async_copy(s_ref.at[me], a_buf.at[0], lsem.at[0])
    own_in.start()

    rows = 2 * capacity
    n1, n2 = 384, 256
    per = width // n1

    def mlp(pair):
        x = a_buf[pl.ds(pair * 2, 2)].reshape(rows, width)
        for n in range(hidden // n1):
            cols = pl.ds(n * n1, n1)
            part = jnp.dot(x, w1_v[:, cols], preferred_element_type=jnp.float32) + b1_ref[:, cols].astype(jnp.float32)
            part = 0.5 * part * (1.0 + lax.erf(part * 0.7071067811865476))
            h_buf[n // per, :, (n % per) * n1:(n % per + 1) * n1] = part.astype(jnp.bfloat16)
        for n in range(0, width, n2):
            h = jnp.concatenate([h_buf[q] for q in range(depth)], axis=1)
            y = jnp.dot(h, w2_v[:, n:n + n2], preferred_element_type=jnp.float32) + b2_ref[:, n:n + n2].astype(jnp.float32)
            a_buf[pl.ds(pair * 2, 2), :, n:n + n2] = y.astype(jnp.bfloat16).reshape(2, capacity, n2)

    own_in.wait()
    w1_copy.wait()
    w2_copy.wait()

    def loop_step(step, carry):
        pair = turn(step)

        @pl.when(step > 0)
        def _():
            send_copy(2 * pair).wait_recv()
        send_copy(2 * pair + 1).wait_recv()
        mlp(pair)

        @pl.when(step > 0)
        def _():
            back_copy(2 * pair + row_c).start()
            back_copy(2 * pair + 1 - row_c).start()

        @pl.when(step == 0)
        def _():
            back_copy(1).start()
        return carry

    lax.fori_loop(0, count // 2, loop_step, 0)
    own_out = pltpu.make_async_copy(a_buf.at[0], r_ref.at[me], lsem.at[1])
    own_out.start()

    route_t = jnp.transpose(wr_ref[...].astype(jnp.float32)).astype(jnp.bfloat16)
    key = key_ref[...].astype(jnp.float32)
    key_unit = key / jnp.sqrt(jnp.sum(key * key, axis=1, keepdims=True))
    for i in range(depth - 1):
        token_load(i).start()

    def gate_step(i, carry):
        @pl.when(i + depth - 1 < chunks)
        def _():
            token_load(i + depth - 1).start()
        token_load(i).wait()
        x = h_buf[lax.rem(i, depth), pl.ds(0, chunk), :]
        proj = lax.dot_general(route_t, x, (((1,), (1,)), ((), ())), preferred_element_type=jnp.float32)
        unit = proj / jnp.sqrt(jnp.sum(proj * proj, axis=0, keepdims=True))
        logits = jnp.dot(key_unit, unit, precision=lax.Precision.HIGHEST, preferred_element_type=jnp.float32) / tau_ref[0, 0]
        weight = jnp.exp(logits - jnp.max(logits, axis=0, keepdims=True))
        cols = pl.ds(pl.multiple_of(i * chunk, chunk), chunk)
        expert = lax.broadcasted_iota(jnp.int32, weight.shape, 0)
        mine = jnp.sum(jnp.where(expert == ids_ref[:, cols], weight, 0.0), axis=0, keepdims=True)
        gate_ref[:, cols] = mine / jnp.sum(weight, axis=0, keepdims=True)
        return carry

    lax.fori_loop(0, chunks, gate_step, 0)
    own_out.wait()

    def drain(k, carry):
        send_copy(k).wait_send()
        copy = back_copy(k)
        copy.wait_send()
        copy.wait_recv()
        return carry

    lax.fori_loop(1, count, drain, 0)


def exchange(tokens, id_row, slot_source, w_route, expert_keys, tau, w_first, b_first, w_second, b_second, nb, na):
    tok_dev, width = tokens.shape
    count = nb * na
    capacity = slot_source.shape[0] // count
    hidden = w_first.shape[1]
    nx = na // 2
    order = send_order(nb, nx)
    any_spec = pl.BlockSpec(memory_space=pl.ANY)
    vmem_spec = pl.BlockSpec(memory_space=pltpu.VMEM)
    smem_spec = pl.BlockSpec(memory_space=pltpu.SMEM)
    flops = 4 * count * capacity * width * hidden
    blocks = jax.ShapeDtypeStruct((count, capacity, width), jnp.bfloat16)
    dma = lambda n: pltpu.SemaphoreType.DMA((n,))
    returned, _, gate = pl.pallas_call(
        functools.partial(exchange_kernel, order, nb, nx),
        name="exchange_mlp",
        out_shape=(blocks, blocks, jax.ShapeDtypeStruct((1, tok_dev), jnp.float32)),
        in_specs=[smem_spec, vmem_spec, smem_spec, any_spec, vmem_spec, vmem_spec, any_spec, vmem_spec, any_spec, vmem_spec],
        out_specs=(any_spec, any_spec, vmem_spec),
        scratch_shapes=[
            pltpu.VMEM((tok_dev * (width // LANES), LANES), jnp.float32),
            pltpu.VMEM((count, capacity, width), jnp.bfloat16),
            pltpu.VMEM((hidden // width, 2 * capacity, width), jnp.bfloat16),
            pltpu.VMEM((width, hidden), jnp.bfloat16),
            pltpu.VMEM((hidden, width), jnp.bfloat16),
            pltpu.VMEM((capacity * (width // LANES), LANES), jnp.float32),
            pltpu.VMEM((2, capacity, width), jnp.bfloat16),
            dma(2), dma(2), dma(hidden // width), dma(2), dma(count), dma(count), dma(count), dma(count),
        ],
        cost_estimate=pl.CostEstimate(flops=flops, bytes_accessed=6 * count * capacity * width, transcendentals=0),
        compiler_params=pltpu.CompilerParams(
            collective_id=0, has_side_effects=True, vmem_limit_bytes=67000000),
    )(slot_source, id_row[None], tau.reshape(1, 1), tokens, w_route, expert_keys,
      w_first, b_first[None], w_second, b_second[None])
    return returned.reshape(count * capacity, width), gate.reshape(tok_dev)


def combine_kernel(dest_ref, gate_ref, back_ref, out_ref, wide, gathered, in_buf, out_buf, in_sem, out_sem):
    slots, width = back_ref.shape
    tokens = out_ref.shape[0]
    parts = width // LANES
    rows = in_buf.shape[1]
    depth = in_buf.shape[0]
    loads = slots // rows

    def load(i):
        return pltpu.make_async_copy(back_ref.at[pl.ds(pl.multiple_of(i * rows, rows), rows)], in_buf.at[lax.rem(i, depth)], in_sem.at[lax.rem(i, depth)])

    for i in range(depth - 1):
        load(i).start()
    wide[pl.ds(slots * parts, 8), :] = jnp.zeros((8, LANES), jnp.float32)

    def widen(i, carry):
        @pl.when(i + depth - 1 < loads)
        def _():
            load(i + depth - 1).start()
        load(i).wait()
        for j in range(parts):
            piece = in_buf[lax.rem(i, depth), :, j * LANES:(j + 1) * LANES].astype(jnp.float32)
            wide[pl.ds(i * rows * parts + j, rows, stride=parts), :] = piece
        return carry

    lax.fori_loop(0, loads, widen, 0)

    def store(i):
        return pltpu.make_async_copy(out_buf.at[lax.rem(i, 2)], out_ref.at[pl.ds(pl.multiple_of(i * rows, rows), rows)], out_sem.at[lax.rem(i, 2)])

    def gather(i, carry):
        def row(r, c):
            base = r * 64
            for q in range(64):
                t = i * rows + base + q
                gathered[pl.ds((base + q) * parts, parts), :] = wide[pl.ds(dest_ref[t] * parts, parts), :] * gate_ref[t]
            return c
        lax.fori_loop(0, rows // 64, row, 0)
        @pl.when(i >= 2)
        def _():
            store(i - 2).wait()
        for j in range(parts):
            out_buf[lax.rem(i, 2), :, j * LANES:(j + 1) * LANES] = gathered[pl.ds(j, rows, stride=parts), :].astype(jnp.bfloat16)
        store(i).start()
        return carry

    lax.fori_loop(0, tokens // rows, gather, 0)
    store(tokens // rows - 2).wait()
    store(tokens // rows - 1).wait()

def combine(back, dest, gate):
    slots, width = back.shape
    tokens = dest.shape[0]
    parts = width // LANES
    rows = 1024
    smem = pl.BlockSpec(memory_space=pltpu.SMEM)
    hbm = pl.BlockSpec(memory_space=pl.ANY)
    return pl.pallas_call(combine_kernel, name="combine",
        out_shape=jax.ShapeDtypeStruct((tokens, width), jnp.bfloat16),
        in_specs=[smem, smem, hbm], out_specs=hbm,
        scratch_shapes=[pltpu.VMEM((slots * parts + 8, LANES), jnp.float32), pltpu.VMEM((rows * parts, LANES), jnp.float32),
            pltpu.VMEM((4, rows, width), jnp.bfloat16), pltpu.VMEM((2, rows, width), jnp.bfloat16),
            pltpu.SemaphoreType.DMA((4,)), pltpu.SemaphoreType.DMA((2,))],
        compiler_params=pltpu.CompilerParams(vmem_limit_bytes=60 * 1024 * 1024))(dest, gate, back)


def solution(mesh):
    nb, na = mesh.shape["ep_b"], mesh.shape["ep_a"]
    num_experts = nb * na
    tok_spec = P(("dp",) + EXPERT_AXES)
    expert_spec = P(EXPERT_AXES)

    def device_step(tokens, expert_ids, route_order, w_route, expert_keys, tau, w_in, b_in, w_out, b_out):
        tok_dev, model_width = tokens.shape[1], tokens.shape[2]
        capacity = (5 * tok_dev + 4 * num_experts - 1) // (4 * num_experts)
        slot_source, dest_slot = route_slots(expert_ids[0], route_order[0], num_experts, capacity)
        returned, gate = exchange(tokens[0], expert_ids[0], slot_source, w_route, expert_keys, tau,
                                  w_in[0], b_in[0], w_out[0], b_out[0], nb, na)
        return combine(returned, dest_slot, gate)[None]

    return jax.shard_map(
        device_step,
        mesh=mesh,
        in_specs=(tok_spec, tok_spec, tok_spec, P(), P(), P(), expert_spec, expert_spec, expert_spec, expert_spec),
        out_specs=tok_spec,
        check_vma=False,
    )
```

```python
import functools

import jax
import jax.numpy as jnp
from jax import lax
from jax.experimental import pallas as pl
from jax.experimental.pallas import tpu as pltpu
from jax.sharding import PartitionSpec as P

EXPERT_AXES = ("ep_b", "ep_a")
MESH = pl.DeviceIdType.MESH
LANES = 128


def hot(values, size):
    return (values[:, None] == jnp.arange(size, dtype=jnp.int32)[None, :]).astype(jnp.bfloat16)


def bdot(a, b):
    return jnp.dot(a, b, preferred_element_type=jnp.float32)


def route_slots(id_row, order_row, num_experts, capacity):
    tok_dev = id_row.shape[0]
    rows = tok_dev // LANES
    slots = num_experts * capacity
    order_hi, order_lo = order_row // LANES, order_row % LANES
    hot_hi, hot_lo = hot(order_hi, rows), hot(order_lo, LANES)
    id_table = id_row.reshape(rows, LANES).astype(jnp.bfloat16)
    ranked_ids = jnp.sum(bdot(hot_hi, id_table) * hot_lo.astype(jnp.float32), axis=1).astype(jnp.int32)
    ranked_hot = hot(ranked_ids, num_experts)
    span = 256
    blocks = ranked_hot.reshape(tok_dev // span, span, num_experts)
    lower = (jnp.arange(span)[:, None] >= jnp.arange(span)[None, :]).astype(jnp.bfloat16)
    within = jnp.einsum("ij,bje->bie", lower, blocks, preferred_element_type=jnp.float32)
    totals = within[:, -1, :]
    before = jnp.cumsum(totals, axis=0) - totals
    ranked_pos = jnp.sum((within + before[:, None, :]) * blocks.astype(jnp.float32), axis=2).reshape(tok_dev)
    ranked_pos = ranked_pos.astype(jnp.int32) - 1
    ranked_slot = jnp.where(ranked_pos < capacity, ranked_ids * capacity + ranked_pos, slots)
    slot_hi, slot_lo = ranked_slot // LANES, ranked_slot % LANES
    as_col = lambda v: v.astype(jnp.bfloat16)[:, None]
    dims = (((0,), (0,)), ((), ()))
    pair = jnp.concatenate([as_col(slot_hi) * hot_lo, as_col(slot_lo) * hot_lo], axis=1)
    table = lax.dot_general(hot_hi, pair, dims, preferred_element_type=jnp.float32).astype(jnp.int32)
    dest_slot = (table[:, :LANES] * LANES + table[:, LANES:]).reshape(tok_dev)
    shot_hi, shot_lo = hot(slot_hi, slots // LANES), hot(slot_lo, LANES)
    pair = jnp.concatenate([as_col(order_hi) * shot_lo, as_col(order_lo) * shot_lo], axis=1)
    table = lax.dot_general(shot_hi, pair, dims, preferred_element_type=jnp.float32).astype(jnp.int32)
    slot_source = (table[:, :LANES] * LANES + table[:, LANES:]).reshape(slots)
    return slot_source, dest_slot


def send_order(nb, nx):
    near = lambda y, x: [(y, x), ((nb - y) % nb, (nx - x) % nx)]
    pair = lambda offs, c: [(y, x, c) for y, x in offs]
    far = lambda y, x: [(y, x, 0), (y, x, 1)]
    hy, hx = nb // 2, nx // 2
    col, row = near(1, 0), near(0, 1)
    same, cross = near(1, 1), near(1, nx - 1)
    x_one, y_one = near(hy, 1), near(1, hx)
    return ([(0, 0, 0), (0, 0, 1)] + pair(col, 0) + pair(col, 1) + far(hy, 0) + pair(same, 0) + pair(same, 1) + pair(cross, 0) + pair(cross, 1) + pair(x_one, 0) + pair(row, 0) + pair(x_one, 1) + pair(row, 1) + far(0, hx) + pair(y_one, 0) + pair(y_one, 1) + far(hy, hx))


def exchange_kernel(order, nb, nx, source_ref, ids_ref, tau_ref, tok_hbm, wr_ref, key_ref, w1_hbm, b1_ref, w2_hbm, b2_ref,
                    r_ref, s_ref, gate_ref, wide, a_buf, h_buf, w1_v, w2_v, gathered, stage,
                    wsem, lsem, tsem, gsem, send1, recv1, send2, recv2):
    count, capacity, width = a_buf.shape
    hidden = w1_v.shape[1]
    tok_dev = tok_hbm.shape[0]
    parts = width // LANES
    row_b, row_a = lax.axis_index("ep_b"), lax.axis_index("ep_a")
    row_x, row_c = row_a // 2, lax.rem(row_a, 2)
    me = row_b * (2 * nx) + row_a

    def peer(y, x, c):
        return lax.rem(row_b + y, nb), lax.rem(row_x + x, nx) * 2 + lax.rem(row_c + c, 2)

    barrier = pltpu.get_barrier_semaphore()
    for y, x, c in order[1:]:
        pb, pa = peer(y, x, c)
        pl.semaphore_signal(barrier, inc=1, device_id={"ep_b": pb, "ep_a": pa}, device_id_type=MESH)

    chunk, depth = 512, h_buf.shape[0]
    chunks = tok_dev // chunk

    def token_load(i):
        slot = lax.rem(i, depth)
        return pltpu.make_async_copy(
            tok_hbm.at[pl.ds(pl.multiple_of(i * chunk, chunk), chunk)], h_buf.at[slot, pl.ds(0, chunk)], tsem.at[slot])

    for i in range(depth - 1):
        token_load(i).start()

    def widen(i, carry):
        @pl.when(i + depth - 1 < chunks)
        def _():
            token_load(i + depth - 1).start()
        token_load(i).wait()
        for j in range(parts):
            piece = h_buf[lax.rem(i, depth), pl.ds(0, chunk), j * LANES:(j + 1) * LANES].astype(jnp.float32)
            wide[pl.ds(i * chunk * parts + j, chunk, stride=parts), :] = piece
        return carry

    lax.fori_loop(0, chunks, widen, 0)
    w1_copy = pltpu.make_async_copy(w1_hbm, w1_v, wsem.at[0])
    w2_copy = pltpu.make_async_copy(w2_hbm, w2_v, wsem.at[1])
    w1_copy.start()
    w2_copy.start()

    words = []
    for w in range(0, count, 5):
        word = 0
        for j, (y, x, c) in enumerate(order[w:w + 5]):
            word += (y * (2 * nx) + x * 2 + c) << (6 * j)
        words.append(word)

    def offset(k):
        word = 0
        for w, value in enumerate(words):
            word = word + jnp.where(k // 5 == w, value, 0)
        code = lax.rem(lax.shift_right_logical(word, 6 * lax.rem(k, 5)), 64)
        return code // (2 * nx), lax.rem(code // 2, nx), lax.rem(code, 2)

    def fill(block, slot):
        def rows16(r, carry):
            for q in range(16):
                src = source_ref[block * capacity + r * 16 + q]
                gathered[pl.ds((r * 16 + q) * parts, parts), :] = wide[pl.ds(src, parts), :]
            return carry
        lax.fori_loop(0, capacity // 16, rows16, 0)
        for j in range(parts):
            stage[slot, :, j * LANES:(j + 1) * LANES] = gathered[pl.ds(j, capacity, stride=parts), :].astype(jnp.bfloat16)

    def stage_copy(k, slot):
        y, x, c = offset(k)
        pb, pa = peer(y, x, c)
        return pltpu.make_async_copy(stage.at[slot], s_ref.at[pb * (2 * nx) + pa], gsem.at[slot])

    def send_copy(k):
        y, x, c = offset(k)
        pb, pa = peer(y, x, c)
        return pltpu.make_async_remote_copy(
            src_ref=s_ref.at[pb * (2 * nx) + pa], dst_ref=a_buf.at[k], send_sem=send1.at[k], recv_sem=recv1.at[k],
            device_id={"ep_b": pb, "ep_a": pa}, device_id_type=MESH)

    def back_copy(k):
        y, x, c = offset(k)
        pb, pa = peer(nb - y, nx - x, c)
        return pltpu.make_async_remote_copy(
            src_ref=a_buf.at[k], dst_ref=r_ref.at[me], send_sem=send2.at[k], recv_sem=recv2.at[k],
            device_id={"ep_b": pb, "ep_a": pa}, device_id_type=MESH)

    def turn(step):
        return step + jnp.where((step // 4) == 2, row_c * (1 - 2 * lax.rem(step, 2)), 0)

    def seq(i):
        return jnp.where(i < 2, i, 2 * turn(i // 2) + lax.rem(i + row_c, 2))

    pl.semaphore_wait(barrier, count - 1)

    def fill_step(i, carry):
        k = seq(i)
        y, x, c = offset(k)
        pb, pa = peer(y, x, c)
        slot = lax.rem(i, 2)
        fill(pb * (2 * nx) + pa, slot)
        stage_copy(k, slot).start()

        @pl.when(i > 1)
        def _():
            before = seq(i - 1)
            stage_copy(before, 1 - slot).wait()
            send_copy(before).start()
        return carry

    lax.fori_loop(1, count, fill_step, 0)
    last = seq(count - 1)
    stage_copy(last, (count - 1) % 2).wait()
    send_copy(last).start()
    fill(me, 0)
    own_in = pltpu.make_async_copy(stage.at[0], s_ref.at[me], lsem.at[0])
    own_in.start()
    own_in.wait()
    own_in = pltpu.make_async_copy(s_ref.at[me], a_buf.at[0], lsem.at[0])
    own_in.start()

    rows = 2 * capacity
    n1, n2 = 384, 256
    per = width // n1

    def mlp(pair):
        x = a_buf[pl.ds(pair * 2, 2)].reshape(rows, width)
        for n in range(hidden // n1):
            cols = pl.ds(n * n1, n1)
            part = jnp.dot(x, w1_v[:, cols], preferred_element_type=jnp.float32) + b1_ref[:, cols].astype(jnp.float32)
            part = 0.5 * part * (1.0 + lax.erf(part * 0.7071067811865476))
            h_buf[n // per, :, (n % per) * n1:(n % per + 1) * n1] = part.astype(jnp.bfloat16)
        for n in range(0, width, n2):
            h = jnp.concatenate([h_buf[q] for q in range(depth)], axis=1)
            y = jnp.dot(h, w2_v[:, n:n + n2], preferred_element_type=jnp.float32) + b2_ref[:, n:n + n2].astype(jnp.float32)
            a_buf[pl.ds(pair * 2, 2), :, n:n + n2] = y.astype(jnp.bfloat16).reshape(2, capacity, n2)

    own_in.wait()
    w1_copy.wait()
    w2_copy.wait()

    def loop_step(step, carry):
        pair = turn(step)

        @pl.when(step > 0)
        def _():
            send_copy(2 * pair).wait_recv()
        send_copy(2 * pair + 1).wait_recv()
        mlp(pair)

        @pl.when(step > 0)
        def _():
            back_copy(2 * pair + row_c).start()
            back_copy(2 * pair + 1 - row_c).start()

        @pl.when(step == 0)
        def _():
            back_copy(1).start()
        return carry

    lax.fori_loop(0, count // 2, loop_step, 0)
    own_out = pltpu.make_async_copy(a_buf.at[0], r_ref.at[me], lsem.at[1])
    own_out.start()

    route_t = jnp.transpose(wr_ref[...].astype(jnp.float32)).astype(jnp.bfloat16)
    key = key_ref[...].astype(jnp.float32)
    key_unit = key / jnp.sqrt(jnp.sum(key * key, axis=1, keepdims=True))
    for i in range(depth - 1):
        token_load(i).start()

    def gate_step(i, carry):
        @pl.when(i + depth - 1 < chunks)
        def _():
            token_load(i + depth - 1).start()
        token_load(i).wait()
        x = h_buf[lax.rem(i, depth), pl.ds(0, chunk), :]
        proj = lax.dot_general(route_t, x, (((1,), (1,)), ((), ())), preferred_element_type=jnp.float32)
        unit = proj / jnp.sqrt(jnp.sum(proj * proj, axis=0, keepdims=True))
        logits = jnp.dot(key_unit, unit, precision=lax.Precision.HIGHEST, preferred_element_type=jnp.float32) / tau_ref[0, 0]
        weight = jnp.exp(logits - jnp.max(logits, axis=0, keepdims=True))
        cols = pl.ds(pl.multiple_of(i * chunk, chunk), chunk)
        expert = lax.broadcasted_iota(jnp.int32, weight.shape, 0)
        mine = jnp.sum(jnp.where(expert == ids_ref[:, cols], weight, 0.0), axis=0, keepdims=True)
        gate_ref[:, cols] = mine / jnp.sum(weight, axis=0, keepdims=True)
        return carry

    lax.fori_loop(0, chunks, gate_step, 0)
    own_out.wait()

    def drain(k, carry):
        send_copy(k).wait_send()
        copy = back_copy(k)
        copy.wait_send()
        copy.wait_recv()
        return carry

    lax.fori_loop(1, count, drain, 0)


def exchange(tokens, id_row, slot_source, w_route, expert_keys, tau, w_first, b_first, w_second, b_second, nb, na):
    tok_dev, width = tokens.shape
    count = nb * na
    capacity = slot_source.shape[0] // count
    hidden = w_first.shape[1]
    nx = na // 2
    order = send_order(nb, nx)
    any_spec = pl.BlockSpec(memory_space=pl.ANY)
    vmem_spec = pl.BlockSpec(memory_space=pltpu.VMEM)
    smem_spec = pl.BlockSpec(memory_space=pltpu.SMEM)
    flops = 4 * count * capacity * width * hidden
    blocks = jax.ShapeDtypeStruct((count, capacity, width), jnp.bfloat16)
    dma = lambda n: pltpu.SemaphoreType.DMA((n,))
    returned, _, gate = pl.pallas_call(
        functools.partial(exchange_kernel, order, nb, nx),
        name="exchange_mlp",
        out_shape=(blocks, blocks, jax.ShapeDtypeStruct((1, tok_dev), jnp.float32)),
        in_specs=[smem_spec, vmem_spec, smem_spec, any_spec, vmem_spec, vmem_spec, any_spec, vmem_spec, any_spec, vmem_spec],
        out_specs=(any_spec, any_spec, vmem_spec),
        scratch_shapes=[
            pltpu.VMEM((tok_dev * (width // LANES), LANES), jnp.float32),
            pltpu.VMEM((count, capacity, width), jnp.bfloat16),
            pltpu.VMEM((hidden // width, 2 * capacity, width), jnp.bfloat16),
            pltpu.VMEM((width, hidden), jnp.bfloat16),
            pltpu.VMEM((hidden, width), jnp.bfloat16),
            pltpu.VMEM((capacity * (width // LANES), LANES), jnp.float32),
            pltpu.VMEM((2, capacity, width), jnp.bfloat16),
            dma(2), dma(2), dma(hidden // width), dma(2), dma(count), dma(count), dma(count), dma(count),
        ],
        cost_estimate=pl.CostEstimate(flops=flops, bytes_accessed=6 * count * capacity * width, transcendentals=0),
        compiler_params=pltpu.CompilerParams(
            collective_id=0, has_side_effects=True, vmem_limit_bytes=67000000),
    )(slot_source * (width // LANES), id_row[None], tau.reshape(1, 1), tokens, w_route, expert_keys,
      w_first, b_first[None], w_second, b_second[None])
    return returned.reshape(count * capacity, width), gate.reshape(tok_dev)


def combine_kernel(dest_ref, gate_ref, back_ref, out_ref, wide, gathered, in_buf, out_buf, in_sem, out_sem):
    slots, width = back_ref.shape
    tokens = out_ref.shape[0]
    parts = width // LANES
    rows = in_buf.shape[1]
    depth = in_buf.shape[0]
    loads = slots // rows

    def load(i):
        return pltpu.make_async_copy(back_ref.at[pl.ds(pl.multiple_of(i * rows, rows), rows)], in_buf.at[lax.rem(i, depth)], in_sem.at[lax.rem(i, depth)])

    for i in range(depth - 1):
        load(i).start()
    wide[pl.ds(slots * parts, 8), :] = jnp.zeros((8, LANES), jnp.float32)

    def widen(i, carry):
        @pl.when(i + depth - 1 < loads)
        def _():
            load(i + depth - 1).start()
        load(i).wait()
        for j in range(parts):
            piece = in_buf[lax.rem(i, depth), :, j * LANES:(j + 1) * LANES].astype(jnp.float32)
            wide[pl.ds(i * rows * parts + j, rows, stride=parts), :] = piece
        return carry

    lax.fori_loop(0, loads, widen, 0)

    def store(i):
        return pltpu.make_async_copy(out_buf.at[lax.rem(i, 2)], out_ref.at[pl.ds(pl.multiple_of(i * rows, rows), rows)], out_sem.at[lax.rem(i, 2)])

    def gather(i, carry):
        def row(r, c):
            base = r * 64
            for q in range(64):
                t = i * rows + base + q
                gathered[pl.ds((base + q) * parts, parts), :] = wide[pl.ds(dest_ref[t], parts), :] * gate_ref[t]
            return c
        lax.fori_loop(0, rows // 64, row, 0)
        @pl.when(i >= 2)
        def _():
            store(i - 2).wait()
        for j in range(parts):
            out_buf[lax.rem(i, 2), :, j * LANES:(j + 1) * LANES] = gathered[pl.ds(j, rows, stride=parts), :].astype(jnp.bfloat16)
        store(i).start()
        return carry

    lax.fori_loop(0, tokens // rows, gather, 0)
    store(tokens // rows - 2).wait()
    store(tokens // rows - 1).wait()

def combine(back, dest, gate):
    slots, width = back.shape
    tokens = dest.shape[0]
    parts = width // LANES
    rows = 1024
    smem = pl.BlockSpec(memory_space=pltpu.SMEM)
    hbm = pl.BlockSpec(memory_space=pl.ANY)
    return pl.pallas_call(combine_kernel, name="combine",
        out_shape=jax.ShapeDtypeStruct((tokens, width), jnp.bfloat16),
        in_specs=[smem, smem, hbm], out_specs=hbm,
        scratch_shapes=[pltpu.VMEM((slots * parts + 8, LANES), jnp.float32), pltpu.VMEM((rows * parts, LANES), jnp.float32),
            pltpu.VMEM((4, rows, width), jnp.bfloat16), pltpu.VMEM((2, rows, width), jnp.bfloat16),
            pltpu.SemaphoreType.DMA((4,)), pltpu.SemaphoreType.DMA((2,))],
        compiler_params=pltpu.CompilerParams(vmem_limit_bytes=60 * 1024 * 1024))(dest * parts, gate, back)


def solution(mesh):
    nb, na = mesh.shape["ep_b"], mesh.shape["ep_a"]
    num_experts = nb * na
    tok_spec = P(("dp",) + EXPERT_AXES)
    expert_spec = P(EXPERT_AXES)

    def device_step(tokens, expert_ids, route_order, w_route, expert_keys, tau, w_in, b_in, w_out, b_out):
        tok_dev, model_width = tokens.shape[1], tokens.shape[2]
        capacity = (5 * tok_dev + 4 * num_experts - 1) // (4 * num_experts)
        slot_source, dest_slot = route_slots(expert_ids[0], route_order[0], num_experts, capacity)
        returned, gate = exchange(tokens[0], expert_ids[0], slot_source, w_route, expert_keys, tau,
                                  w_in[0], b_in[0], w_out[0], b_out[0], nb, na)
        return combine(returned, dest_slot, gate)[None]

    return jax.shard_map(
        device_step,
        mesh=mesh,
        in_specs=(tok_spec, tok_spec, tok_spec, P(), P(), P(), expert_spec, expert_spec, expert_spec, expert_spec),
        out_specs=tok_spec,
        check_vma=False,
    )
```
